32 devices in a mesh: dp: 4 (over y, core), seq: 8 (over z, x).
Axes of the slice: x: 2, y: 2, z: 4, core: 2. Of those that a mesh axis runs over, the one named last changes fastest.
Arguments:
- queries: bfloat16 [32, 2048, 512], P('dp', 'seq'), may hold values from -6 to 6
- enc_keys: bfloat16 [32, 2048, 512], P('dp', 'seq'), may hold values from -6 to 6
- enc_values: bfloat16 [32, 2048, 512], P('dp', 'seq'), may hold values from -6 to 6
- dec_ids: int32 [32, 2048], P('dp', 'seq'), may hold values from 0 to 15, never falling along the last dimension, each value on 1 to 512 neighbouring positions
- enc_ids: int32 [32, 2048], P('dp', 'seq'), may hold values from 0 to 15, never falling along the last dimension, each value on 1 to 512 neighbouring positions
Outputs:
- context: bfloat16 [32, 2048, 512], P('dp', 'seq')
The draws below stay inside these ranges and needn't reach their ends.
Inputs may be any that keep to these rules, and one draw needn't show every extreme that they name: `dec_ids`: along each row the numbers never fall; every number from 0 to 15 occurs in every row; a document holds 1 to 512 positions of a row, and some document holds exactly 512. `enc_ids`: along each row the numbers never fall; every number from 0 to 15 occurs in every row; a document holds 1 to 512 positions of a row, and some document holds exactly 512.
All inputs are finite; a program needn't handle non-finite values.
Results may differ from the reference program's by a relative error of at most 0.0047.
Values may be sent and summed in bfloat16 or wider, within the bound.
A program may use at most 128 MiB of HBM per device.

```python
import math
import jax
import jax.numpy as jnp
import numpy as np
from jax import lax

HEAD_DIM = 64
LEN = 2048
NDOC = 16
MOST = 512
HEADS = 8
INNER = 512
BATCH = 32


def draw_queries(key, part):
    base = jax.random.truncated_normal(jax.random.fold_in(key, 1), -6.0, 6.0, (BATCH, LEN, HEADS * HEAD_DIM), jnp.float32)
    result = 0.25 * base
    return result.astype(jnp.bfloat16)


def draw_enc_keys(key, part):
    base = jax.random.truncated_normal(jax.random.fold_in(key, 3), -6.0, 6.0, (BATCH, LEN, HEADS * HEAD_DIM), jnp.float32)
    result = base
    return result.astype(jnp.bfloat16)


def levels(rng, dims, cuts, least, top_value):
    level, own = 1.0, jax.random.fold_in(rng, 6)
    for dim, parts in cuts:
        heights = jnp.exp(jax.random.uniform(jax.random.fold_in(own, dim), (parts,), jnp.float32, least / len(cuts), top_value / len(cuts)))
        level = level * jnp.repeat(heights, dims[dim] // parts).reshape([-1 if axis == dim else 1 for axis in range(len(dims))])
    return level


def split_up(amount, total, most, lean):
    weights = [(1 << 20) // math.isqrt(grade ** lean) + 1 for grade in range(2, amount + 1)]
    surplus, given = total - most - (amount - 1), [1] * (amount - 1)
    while surplus > 0:
        free = [i for i in range(amount - 1) if given[i] < most]
        pool, left = sum([weights[i] for i in free]), surplus
        for i in free:
            addition = min(most - given[i], max(1, left * weights[i] // pool), surplus)
            given[i] = given[i] + addition
            surplus = surplus - addition
    return np.array([most] + given)


def uneven_parts(stream_key, number_of, total, most, slope):
    if number_of == 2:
        one = jax.random.randint(stream_key, (), max(1, total - most), min(most, total - 1) + 1)
        return jnp.stack([one, total - one])
    sizes = jnp.asarray(split_up(number_of, total, most, slope), jnp.int32)
    pairs = (number_of - 1) // 2
    giver, sink = sizes[1:1 + 2 * pairs:2], sizes[2:2 + 2 * pairs:2]
    slack = jnp.minimum(giver - 1, most - sink)
    moved = jax.random.randint(jax.random.fold_in(stream_key, 1), (pairs,), 0, 1 << 20) % (slack + 1)
    sizes = sizes.at[1:1 + 2 * pairs:2].set(giver - moved).at[2:2 + 2 * pairs:2].set(sink + moved)
    return sizes[jax.random.permutation(jax.random.fold_in(stream_key, 2), number_of)]


def scatter_about(key, extent, scale, reach, shards=(), kind=jnp.bfloat16):
    factor_of = levels(key, extent, shards, -0.22, 0.18) if shards else 1.0
    values = jax.random.normal(key, extent, jnp.float32) * scale * factor_of
    return jnp.minimum(jnp.maximum(values, -reach), reach).astype(kind)


def setup_inputs(seed: int = 0) -> dict:
    splits = jax.random.split(jax.random.key(seed), 6)
    return {
        "queries": draw_queries(jax.random.fold_in(splits[5], 71), 0),
        "enc_keys": draw_enc_keys(jax.random.fold_in(splits[5], 71), 0),
        "enc_values": scatter_about(splits[2], (BATCH, LEN, INNER), 1.0, 6.0, ((0, 4), (1, 8))),
        "dec_ids": jax.vmap(lambda own: jnp.searchsorted(jnp.cumsum(uneven_parts(own, NDOC, LEN, MOST, 2)), jnp.arange(LEN), side="right"))(jax.random.split(splits[3], BATCH)).reshape((BATCH, LEN)).astype(jnp.int32),
        "enc_ids": jax.vmap(lambda own: jnp.searchsorted(jnp.cumsum(uneven_parts(own, NDOC, LEN, MOST, 2)), jnp.arange(LEN), side="right"))(jax.random.split(splits[4], BATCH)).reshape((BATCH, LEN)).astype(jnp.int32),
    }


masked_score = -1.0e30


def attend_row(query_row, key_row, value_row, dec_row, enc_row):
    query_heads = query_row.astype(jnp.float32).reshape(LEN, HEADS, HEAD_DIM)
    key_heads = key_row.astype(jnp.float32).reshape(LEN, HEADS, HEAD_DIM)
    value_heads = value_row.astype(jnp.float32).reshape(LEN, HEADS, HEAD_DIM)
    query_span = min(512, LEN)
    pieces = []
    for offset in range(0, LEN, query_span):
        scores = jnp.einsum("qhd,khd->hqk", query_heads[offset:offset + query_span], key_heads,
                            precision=lax.Precision.HIGHEST)
        allowed = (dec_row[offset:offset + query_span][:, None] == enc_row[None, :])[None]
        scores = jnp.where(allowed, scores, masked_score)
        row_peak = jnp.max(scores, axis=2, keepdims=True)
        expos = jnp.where(allowed, jnp.exp(scores - row_peak), 0.0)
        row_total = jnp.sum(expos, axis=2, keepdims=True)
        weights = (expos / row_total).astype(jnp.bfloat16)
        weights = lax.optimization_barrier(weights).astype(jnp.float32)
        summed = jnp.einsum("hqk,khd->qhd", weights, value_heads, precision=lax.Precision.HIGHEST)
        pieces.append(summed.reshape(query_span, HEADS * HEAD_DIM).astype(jnp.bfloat16))
    return jnp.concatenate(pieces, axis=0)


def reference(queries, enc_keys, enc_values, dec_ids, enc_ids):
    def one_row(members):
        return attend_row(members[0], members[1], members[2], members[3], members[4])

    return lax.map(one_row, (queries, enc_keys, enc_values, dec_ids, enc_ids))
```

```python
import functools

import jax
import jax.numpy as jnp
from jax import lax
from jax.experimental import pallas as pl
from jax.experimental.pallas import tpu as pltpu
from jax.sharding import PartitionSpec as P

HEAD_DIM = 64
DOCS = 16
CHUNKS = 4
SPAN = 256
MASKED = -8192.0


def pack_kernel(q_ref, k_ref, v_ref, o_ref):
    group, _, _, width, count = o_ref.shape
    for slot, ref in enumerate((q_ref, k_ref, v_ref)):
        o_ref[:, slot, 0] = ref[0].T.reshape(group, width, count)


def pack(q, k, v, group, first, rows):
    _, count, features = q.shape
    width = features // group
    spec = pl.BlockSpec((1, count, features), lambda r: (r + first, 0, 0))
    return pl.pallas_call(
        pack_kernel,
        grid=(rows,),
        in_specs=[spec] * 3,
        out_specs=pl.BlockSpec((group, 3, 1, width, count), lambda r: (0, 0, r, 0, 0)),
        out_shape=jax.ShapeDtypeStruct((group, 3, rows, width, count), q.dtype),
        cost_estimate=pl.CostEstimate(
            flops=4 * rows * count * features, bytes_accessed=12 * rows * count * features, transcendentals=0
        ),
    )(q, k, v)


def unpack_kernel(x_ref, *rest):
    o_ref = rest[-1]
    group, _, width, count = x_ref.shape
    o_ref[0] = x_ref[:, 0].reshape(group * width, count).T


def unpack(x, held, first, total):
    group, rows, width, count = x.shape
    args = (x,) if held is None else (x, held)
    in_specs = [pl.BlockSpec((group, 1, width, count), lambda r: (0, r, 0, 0))]
    if held is not None:
        in_specs.append(pl.BlockSpec(memory_space=pl.ANY))
    return pl.pallas_call(
        unpack_kernel,
        grid=(rows,),
        in_specs=in_specs,
        out_specs=pl.BlockSpec((1, count, group * width), lambda r: (r + first, 0, 0)),
        out_shape=jax.ShapeDtypeStruct((total, count, group * width), x.dtype),
        input_output_aliases={} if held is None else {1: 0},
        cost_estimate=pl.CostEstimate(
            flops=4 * rows * count * group * width, bytes_accessed=4 * rows * count * group * width, transcendentals=0
        ),
    )(*args)


def attend_kernel(heads, low_ref, high_ref, x_ref, dec_ref, enc_ref, o_ref, q_all, k_all, v_all):
    group, _, _, width, count = x_ref.shape
    length = group * count
    row = pl.program_id(0)
    span = min(SPAN, length)
    documents = lax.broadcasted_iota(jnp.int32, (DOCS, length), 0)
    dec_hot = jnp.where(documents == dec_ref[0], 1.0, 0.0).astype(jnp.bfloat16)
    enc_miss = jnp.where(documents == enc_ref[0], 0.0, MASKED).astype(jnp.bfloat16)
    for head in range(heads):
        place = pl.ds(head * HEAD_DIM, HEAD_DIM)
        for part in range(group):
            columns = pl.ds(part * count, count)
            q_all[:HEAD_DIM, columns] = x_ref[part, 0, 0, place]
            v_all[:, columns] = x_ref[part, 2, 0, place]
        q_all[HEAD_DIM:, :] = dec_hot
        for part in range(group):
            columns = slice(part * count, (part + 1) * count)
            both = jnp.concatenate([x_ref[part, 1, 0, place], enc_miss[:, columns]], axis=0)
            k_all[columns, :] = both.T

        def one_span(block):
            at = pl.multiple_of(block * span, span)
            query = q_all[:, pl.ds(at, span)]
            low = low_ref[row, block]
            steps = high_ref[row, block]

            def step(index, held):
                peak, total, summed = held
                start = pl.multiple_of(low + index * span, 128)
                scores = jnp.dot(
                    k_all[pl.ds(start, span), :], query, preferred_element_type=jnp.float32
                )
                fresh = jnp.maximum(peak, jnp.max(scores, axis=0, keepdims=True))
                scale = jnp.exp(peak - fresh)
                expos = jnp.exp(scores - fresh)
                total = total * scale + jnp.sum(expos, axis=0, keepdims=True)
                summed = summed * scale + jnp.dot(
                    v_all[:, pl.ds(start, span)], expos.astype(jnp.bfloat16), preferred_element_type=jnp.float32
                )
                return fresh, total, summed

            init = (
                jnp.full((1, span), 4 * MASKED, jnp.float32),
                jnp.zeros((1, span), jnp.float32),
                jnp.zeros((HEAD_DIM, span), jnp.float32),
            )
            _, total, summed = lax.fori_loop(0, steps, step, init)
            return (summed / total).astype(jnp.bfloat16)

        if count == span:

            def each(block, carry):
                o_ref[block, 0, place] = one_span(block)
                return carry

            lax.fori_loop(0, length // span, each, 0)
        else:
            for block in range(length // span):
                result = one_span(block)
                for piece in range(0, span, count):
                    at = block * span + piece
                    width_here = min(count, span)
                    o_ref[at // count, 0, place, pl.ds(at % count, width_here)] = result[:, piece : piece + width_here]


def tables(dec_rows, enc_rows):
    rows, length = dec_rows.shape
    span = min(SPAN, length)
    docs = dec_rows.reshape(rows, length // span, span)
    before = jnp.sum(enc_rows[:, None, :] < docs[:, :, :1], axis=2, dtype=jnp.int32)
    upto = jnp.sum(enc_rows[:, None, :] <= docs[:, :, -1:], axis=2, dtype=jnp.int32)
    low = before // 128 * 128
    steps = (upto - low + span - 1) // span
    return jnp.minimum(low, length - steps * span), steps


def attend(x, low, steps, dec_rows, enc_rows):
    group, _, rows, width, count = x.shape
    length = group * count
    heads = width // HEAD_DIM
    return pl.pallas_call(
        functools.partial(attend_kernel, heads),
        grid_spec=pltpu.PrefetchScalarGridSpec(
            num_scalar_prefetch=2,
            grid=(rows,),
            in_specs=[
                pl.BlockSpec((group, 3, 1, width, count), lambda r, *_: (0, 0, r, 0, 0)),
                pl.BlockSpec((1, 1, length), lambda r, *_: (r, 0, 0)),
                pl.BlockSpec((1, 1, length), lambda r, *_: (r, 0, 0)),
            ],
            out_specs=pl.BlockSpec((group, 1, width, count), lambda r, *_: (0, r, 0, 0)),
            scratch_shapes=[
                pltpu.VMEM((HEAD_DIM + DOCS, length), jnp.bfloat16),
                pltpu.VMEM((length, HEAD_DIM + DOCS), jnp.bfloat16),
                pltpu.VMEM((HEAD_DIM, length), jnp.bfloat16),
            ],
        ),
        out_shape=jax.ShapeDtypeStruct((group, rows, width, count), x.dtype),
        cost_estimate=pl.CostEstimate(
            flops=rows * heads * length * length * 128,
            bytes_accessed=8 * rows * width * length,
            transcendentals=rows * heads * length * length // 4,
        ),
    )(low, steps, x, dec_rows[:, None, :], enc_rows[:, None, :])


def local(queries, enc_keys, enc_values, dec_ids, enc_ids):
    group = lax.axis_size("seq")
    rows, count, _ = queries.shape
    chunks = CHUNKS if rows % CHUNKS == 0 else 1
    each = rows // chunks
    ids = lax.all_gather(jnp.stack([dec_ids, enc_ids]), "seq", axis=2, tiled=True)
    known = (*tables(ids[0], ids[1]), ids[0], ids[1])

    def exchange(block):
        return lax.all_to_all(block, "seq", split_axis=0, concat_axis=0, tiled=True)

    packed = [pack(queries, enc_keys, enc_values, group, chunk * each, each) for chunk in range(chunks)]
    arrived = [None] * chunks
    attended = [None] * chunks
    arrived[0] = exchange(packed[0])
    if chunks > 1:
        packed[1], known = lax.optimization_barrier((packed[1], known))
        arrived[1] = exchange(packed[1])
    for chunk in range(chunks):
        mine = slice(chunk * each, (chunk + 1) * each)
        attended[chunk] = attend(arrived[chunk], *[table[mine] for table in known])
        if chunk + 2 < chunks:
            packed[chunk + 2], attended[chunk] = lax.optimization_barrier((packed[chunk + 2], attended[chunk]))
            arrived[chunk + 2] = exchange(packed[chunk + 2])
        if chunk + 2 == chunks:
            attended[0], arrived[-1] = lax.optimization_barrier((attended[0], arrived[-1]))
    out = None
    for chunk in range(chunks):
        out = unpack(exchange(attended[chunk]), out, chunk * each, rows)
    return out


def solution(mesh):
    in_specs = (
        P("dp", "seq", None),
        P("dp", "seq", None),
        P("dp", "seq", None),
        P("dp", "seq"),
        P("dp", "seq"),
    )
    out_specs = P("dp", "seq", None)
    return jax.shard_map(local, mesh=mesh, in_specs=in_specs, out_specs=out_specs, check_vma=False)
```

```python
import functools

import jax
import jax.numpy as jnp
from jax import lax
from jax.experimental import pallas as pl
from jax.experimental.pallas import tpu as pltpu
from jax.sharding import PartitionSpec as P

HEAD_DIM = 64
DOCS = 16
SPAN = 256
MASKED = -8192.0


def pack_kernel(rows, q_ref, k_ref, v_ref, ids_ref, o_ref):
    group, _, count = o_ref.shape
    width = q_ref.shape[2] // group

    @pl.when(pl.program_id(0) < rows)
    def _():
        for slot, ref in enumerate((q_ref, k_ref, v_ref)):
            o_ref[:, slot * width : (slot + 1) * width] = ref[0].T.reshape(group, width, count)

    @pl.when(pl.program_id(0) == rows)
    def _():
        for target in range(group):
            o_ref[target, : ids_ref.shape[0]] = ids_ref[...]


def pack(q, k, v, ids, group, first, rows, with_ids):
    _, count, features = q.shape
    width = features // group
    spec = pl.BlockSpec((1, count, features), lambda r: (jnp.minimum(r, rows - 1) + first, 0, 0))
    more = ids.shape[0] if with_ids else 0
    return pl.pallas_call(
        functools.partial(pack_kernel, rows),
        grid=(rows + 1 if with_ids else rows,),
        in_specs=[spec] * 3 + [pl.BlockSpec(ids.shape, lambda r: (0, 0))],
        out_specs=pl.BlockSpec((group, 3 * width, count), lambda r: (0, r, 0)),
        out_shape=jax.ShapeDtypeStruct((group, rows * 3 * width + more, count), q.dtype),
        cost_estimate=pl.CostEstimate(
            flops=4 * rows * count * features, bytes_accessed=12 * rows * count * features, transcendentals=0
        ),
    )(q, k, v, ids)


def unpack_kernel(x_ref, *rest):
    o_ref = rest[-1]
    group, _, width, count = x_ref.shape
    o_ref[0] = x_ref[:, 0].reshape(group * width, count).T


def unpack(x, held, first, total):
    group, rows, width, count = x.shape
    args = (x,) if held is None else (x, held)
    in_specs = [pl.BlockSpec((group, 1, width, count), lambda r: (0, r, 0, 0))]
    if held is not None:
        in_specs.append(pl.BlockSpec(memory_space=pl.ANY))
    return pl.pallas_call(
        unpack_kernel,
        grid=(rows,),
        in_specs=in_specs,
        out_specs=pl.BlockSpec((1, count, group * width), lambda r: (r + first, 0, 0)),
        out_shape=jax.ShapeDtypeStruct((total, count, group * width), x.dtype),
        input_output_aliases={} if held is None else {1: 0},
        cost_estimate=pl.CostEstimate(
            flops=4 * rows * count * group * width, bytes_accessed=4 * rows * count * group * width, transcendentals=0
        ),
    )(*args)


def attend_kernel(heads, low_ref, high_ref, x_ref, dec_ref, enc_ref, o_ref, q_all, k_all, v_all):
    group, stacked, count = x_ref.shape
    width = stacked // 3
    length = group * count
    row = pl.program_id(0)
    span = min(SPAN, length)
    documents = lax.broadcasted_iota(jnp.int32, (DOCS, length), 0)
    dec_hot = jnp.where(documents == dec_ref[0], 1.0, 0.0).astype(jnp.bfloat16)
    enc_miss = jnp.where(documents == enc_ref[0], 0.0, MASKED).astype(jnp.bfloat16)
    for head in range(heads):
        place = pl.ds(head * HEAD_DIM, HEAD_DIM)
        for part in range(group):
            columns = pl.ds(part * count, count)
            q_all[:HEAD_DIM, columns] = x_ref[part, place]
            v_all[:, columns] = x_ref[part, pl.ds(2 * width + head * HEAD_DIM, HEAD_DIM)]
        q_all[HEAD_DIM:, :] = dec_hot
        for part in range(group):
            columns = slice(part * count, (part + 1) * count)
            both = jnp.concatenate([x_ref[part, pl.ds(width + head * HEAD_DIM, HEAD_DIM)], enc_miss[:, columns]], axis=0)
            k_all[columns, :] = both.T

        def one_span(block):
            at = pl.multiple_of(block * span, span)
            query = q_all[:, pl.ds(at, span)]
            low = low_ref[row, block]
            steps = high_ref[row, block]

            def step(index, held):
                peak, total, summed = held
                start = pl.multiple_of(low + index * span, 128)
                scores = jnp.dot(
                    k_all[pl.ds(start, span), :], query, preferred_element_type=jnp.float32
                )
                fresh = jnp.maximum(peak, jnp.max(scores, axis=0, keepdims=True))
                scale = jnp.exp(peak - fresh)
                expos = jnp.exp(scores - fresh)
                total = total * scale + jnp.sum(expos, axis=0, keepdims=True)
                summed = summed * scale + jnp.dot(
                    v_all[:, pl.ds(start, span)], expos.astype(jnp.bfloat16), preferred_element_type=jnp.float32
                )
                return fresh, total, summed

            init = (
                jnp.full((1, span), 4 * MASKED, jnp.float32),
                jnp.zeros((1, span), jnp.float32),
                jnp.zeros((HEAD_DIM, span), jnp.float32),
            )
            _, total, summed = lax.fori_loop(0, steps, step, init)
            return (summed / total).astype(jnp.bfloat16)

        if count == span:

            def each(block, carry):
                o_ref[block, 0, place] = one_span(block)
                return carry

            lax.fori_loop(0, length // span, each, 0)
        else:
            for block in range(length // span):
                result = one_span(block)
                for piece in range(0, span, count):
                    at = block * span + piece
                    width_here = min(count, span)
                    o_ref[at // count, 0, place, pl.ds(at % count, width_here)] = result[:, piece : piece + width_here]


def tables(dec_rows, enc_rows):
    rows, length = dec_rows.shape
    span = min(SPAN, length)
    docs = dec_rows.reshape(rows, length // span, span)
    before = jnp.sum(enc_rows[:, None, :] < docs[:, :, :1], axis=2, dtype=jnp.int32)
    upto = jnp.sum(enc_rows[:, None, :] <= docs[:, :, -1:], axis=2, dtype=jnp.int32)
    low = before // 128 * 128
    steps = (upto - low + span - 1) // span
    return jnp.minimum(low, length - steps * span), steps


def attend(x, width, low, steps, dec_rows, enc_rows):
    group, _, count = x.shape
    rows = low.shape[0]
    length = group * count
    heads = width // HEAD_DIM
    return pl.pallas_call(
        functools.partial(attend_kernel, heads),
        grid_spec=pltpu.PrefetchScalarGridSpec(
            num_scalar_prefetch=2,
            grid=(rows,),
            in_specs=[
                pl.BlockSpec((group, 3 * width, count), lambda r, *_: (0, r, 0)),
                pl.BlockSpec((1, 1, length), lambda r, *_: (r, 0, 0)),
                pl.BlockSpec((1, 1, length), lambda r, *_: (r, 0, 0)),
            ],
            out_specs=pl.BlockSpec((group, 1, width, count), lambda r, *_: (0, r, 0, 0)),
            scratch_shapes=[
                pltpu.VMEM((HEAD_DIM + DOCS, length), jnp.bfloat16),
                pltpu.VMEM((length, HEAD_DIM + DOCS), jnp.bfloat16),
                pltpu.VMEM((HEAD_DIM, length), jnp.bfloat16),
            ],
        ),
        out_shape=jax.ShapeDtypeStruct((group, rows, width, count), x.dtype),
        cost_estimate=pl.CostEstimate(
            flops=rows * heads * length * length * 128,
            bytes_accessed=8 * rows * width * length,
            transcendentals=rows * heads * length * length // 4,
        ),
    )(low, steps, x, dec_rows[:, None, :], enc_rows[:, None, :])


def local(queries, enc_keys, enc_values, dec_ids, enc_ids):
    group = lax.axis_size("seq")
    rows, count, features = queries.shape
    width = features // group
    early = max(1, rows * 5 // 8)
    cuts = [(0, early), (early, rows - early)] if rows > 1 else [(0, rows)]
    ids = jnp.concatenate([dec_ids, enc_ids], axis=0).astype(queries.dtype)

    def exchange(block):
        return lax.all_to_all(block, "seq", split_axis=0, concat_axis=0, tiled=True)

    arrived = [
        exchange(pack(queries, enc_keys, enc_values, ids, group, first, size, first == 0)) for first, size in cuts
    ]
    spread = arrived[0][:, early * 3 * width :].astype(jnp.int32)
    whole_rows = spread.transpose(1, 0, 2).reshape(2 * rows, group * count)
    dec_rows, enc_rows = whole_rows[:rows], whole_rows[rows:]
    known = (*tables(dec_rows, enc_rows), dec_rows, enc_rows)
    out = None
    for (first, size), block in zip(cuts, arrived):
        attended = attend(block, width, *[table[first : first + size] for table in known])
        out = unpack(exchange(attended), out, first, rows)
    return out


def solution(mesh):
    in_specs = (
        P("dp", "seq", None),
        P("dp", "seq", None),
        P("dp", "seq", None),
        P("dp", "seq"),
        P("dp", "seq"),
    )
    out_specs = P("dp", "seq", None)
    return jax.shard_map(local, mesh=mesh, in_specs=in_specs, out_specs=out_specs, check_vma=False)
```

```python
import functools

import jax
import jax.numpy as jnp
from jax import lax
from jax.experimental import pallas as pl
from jax.experimental.pallas import tpu as pltpu
from jax.sharding import PartitionSpec as P

HEAD_DIM = 64
DOCS = 16
SPAN = 256
MASKED = -8192.0


def pack_kernel(rows, q_ref, k_ref, v_ref, ids_ref, o_ref):
    group, _, count = o_ref.shape
    width = q_ref.shape[2] // group

    @pl.when(pl.program_id(0) < rows)
    def _():
        for slot, ref in enumerate((q_ref, k_ref, v_ref)):
            o_ref[:, slot * width : (slot + 1) * width] = ref[0].T.reshape(group, width, count)

    @pl.when(pl.program_id(0) == rows)
    def _():
        for target in range(group):
            o_ref[target, : ids_ref.shape[0]] = ids_ref[...]


def pack(q, k, v, ids, group, first, rows, with_ids):
    _, count, features = q.shape
    width = features // group
    spec = pl.BlockSpec((1, count, features), lambda r: (jnp.minimum(r, rows - 1) + first, 0, 0))
    more = ids.shape[0] if with_ids else 0
    return pl.pallas_call(
        functools.partial(pack_kernel, rows),
        grid=(rows + 1 if with_ids else rows,),
        in_specs=[spec] * 3 + [pl.BlockSpec(ids.shape, lambda r: (0, 0))],
        out_specs=pl.BlockSpec((group, 3 * width, count), lambda r: (0, r, 0)),
        out_shape=jax.ShapeDtypeStruct((group, rows * 3 * width + more, count), q.dtype),
        cost_estimate=pl.CostEstimate(
            flops=4 * rows * count * features, bytes_accessed=12 * rows * count * features, transcendentals=0
        ),
    )(q, k, v, ids)


def deliver_kernel(group, x_ref, q_ref, k_ref, v_ref, o_ref, p_ref, held, own_sem, send_sem, recv_sem):
    me = lax.axis_index("seq")

    def transfer(shift):
        target = lax.rem(me + shift, group)
        return pltpu.make_async_remote_copy(
            src_ref=x_ref.at[target],
            dst_ref=o_ref.at[me],
            send_sem=send_sem.at[shift - 1],
            recv_sem=recv_sem.at[shift - 1],
            device_id={"seq": target},
            device_id_type=pl.DeviceIdType.MESH,
        )

    @pl.when(pl.program_id(0) == 0)
    def _():
        barrier = pltpu.get_barrier_semaphore()
        for shift in range(1, group):
            pl.semaphore_signal(
                barrier, inc=1, device_id={"seq": lax.rem(me + shift, group)}, device_id_type=pl.DeviceIdType.MESH
            )
        pl.semaphore_wait(barrier, group - 1)
        for shift in range(1, group):
            transfer(shift).start()
        own = pltpu.make_async_copy(x_ref.at[me], held, own_sem)
        own.start()
        own.wait()
        own = pltpu.make_async_copy(held, o_ref.at[me], own_sem)
        own.start()
        own.wait()

    _, _, count = p_ref.shape
    width = q_ref.shape[2] // group
    for slot, ref in enumerate((q_ref, k_ref, v_ref)):
        p_ref[:, slot * width : (slot + 1) * width] = ref[0].T.reshape(group, width, count)

    @pl.when(pl.program_id(0) == pl.num_programs(0) - 1)
    def _():
        for shift in range(1, group):
            transfer(shift).wait()


def deliver(x, q, k, v, first, rows):
    group = x.shape[0]
    _, count, features = q.shape
    width = features // group
    spec = pl.BlockSpec((1, count, features), lambda r: (r + first, 0, 0))
    return pl.pallas_call(
        functools.partial(deliver_kernel, group),
        grid=(rows,),
        in_specs=[pl.BlockSpec(memory_space=pl.ANY)] + [spec] * 3,
        out_specs=(
            pl.BlockSpec(memory_space=pl.ANY),
            pl.BlockSpec((group, 3 * width, count), lambda r: (0, r, 0)),
        ),
        out_shape=(
            jax.ShapeDtypeStruct(x.shape, x.dtype),
            jax.ShapeDtypeStruct((group, rows * 3 * width, count), x.dtype),
        ),
        scratch_shapes=[
            pltpu.VMEM(x.shape[1:], x.dtype),
            pltpu.SemaphoreType.DMA,
            pltpu.SemaphoreType.DMA((group - 1,)),
            pltpu.SemaphoreType.DMA((group - 1,)),
        ],
        compiler_params=pltpu.CompilerParams(collective_id=0, has_side_effects=True),
    )(x, q, k, v)


def unpack_kernel(x_ref, *rest):
    o_ref = rest[-1]
    group, _, width, count = x_ref.shape
    o_ref[0] = x_ref[:, 0].reshape(group * width, count).T


def unpack(x, held, first, total):
    group, rows, width, count = x.shape
    args = (x,) if held is None else (x, held)
    in_specs = [pl.BlockSpec((group, 1, width, count), lambda r: (0, r, 0, 0))]
    if held is not None:
        in_specs.append(pl.BlockSpec(memory_space=pl.ANY))
    return pl.pallas_call(
        unpack_kernel,
        grid=(rows,),
        in_specs=in_specs,
        out_specs=pl.BlockSpec((1, count, group * width), lambda r: (r + first, 0, 0)),
        out_shape=jax.ShapeDtypeStruct((total, count, group * width), x.dtype),
        input_output_aliases={} if held is None else {1: 0},
        cost_estimate=pl.CostEstimate(
            flops=4 * rows * count * group * width, bytes_accessed=4 * rows * count * group * width, transcendentals=0
        ),
    )(*args)


def attend_kernel(heads, low_ref, high_ref, x_ref, dec_ref, enc_ref, o_ref, q_all, k_all, v_all):
    group, stacked, count = x_ref.shape
    width = stacked // 3
    length = group * count
    row = pl.program_id(0)
    span = min(SPAN, length)
    documents = lax.broadcasted_iota(jnp.int32, (DOCS, length), 0)
    dec_hot = jnp.where(documents == dec_ref[0], 1.0, 0.0).astype(jnp.bfloat16)
    enc_miss = jnp.where(documents == enc_ref[0], 0.0, MASKED).astype(jnp.bfloat16)
    for head in range(heads):
        place = pl.ds(head * HEAD_DIM, HEAD_DIM)
        for part in range(group):
            columns = pl.ds(part * count, count)
            q_all[:HEAD_DIM, columns] = x_ref[part, place]
            v_all[:, columns] = x_ref[part, pl.ds(2 * width + head * HEAD_DIM, HEAD_DIM)]
        q_all[HEAD_DIM:, :] = dec_hot
        for part in range(group):
            columns = slice(part * count, (part + 1) * count)
            both = jnp.concatenate([x_ref[part, pl.ds(width + head * HEAD_DIM, HEAD_DIM)], enc_miss[:, columns]], axis=0)
            k_all[columns, :] = both.T

        def one_span(block):
            at = pl.multiple_of(block * span, span)
            query = q_all[:, pl.ds(at, span)]
            low = low_ref[row, block]
            steps = high_ref[row, block]

            def step(index, held):
                peak, total, summed = held
                start = pl.multiple_of(low + index * span, 128)
                scores = jnp.dot(
                    k_all[pl.ds(start, span), :], query, preferred_element_type=jnp.float32
                )
                fresh = jnp.maximum(peak, jnp.max(scores, axis=0, keepdims=True))
                scale = jnp.exp(peak - fresh)
                expos = jnp.exp(scores - fresh)
                total = total * scale + jnp.sum(expos, axis=0, keepdims=True)
                summed = summed * scale + jnp.dot(
                    v_all[:, pl.ds(start, span)], expos.astype(jnp.bfloat16), preferred_element_type=jnp.float32
                )
                return fresh, total, summed

            init = (
                jnp.full((1, span), 4 * MASKED, jnp.float32),
                jnp.zeros((1, span), jnp.float32),
                jnp.zeros((HEAD_DIM, span), jnp.float32),
            )
            _, total, summed = lax.fori_loop(0, steps, step, init)
            return (summed / total).astype(jnp.bfloat16)

        if count == span:

            def each(block, carry):
                o_ref[block, 0, place] = one_span(block)
                return carry

            lax.fori_loop(0, length // span, each, 0)
        else:
            for block in range(length // span):
                result = one_span(block)
                for piece in range(0, span, count):
                    at = block * span + piece
                    width_here = min(count, span)
                    o_ref[at // count, 0, place, pl.ds(at % count, width_here)] = result[:, piece : piece + width_here]


def tables(dec_rows, enc_rows):
    rows, length = dec_rows.shape
    span = min(SPAN, length)
    docs = dec_rows.reshape(rows, length // span, span)
    before = jnp.sum(enc_rows[:, None, :] < docs[:, :, :1], axis=2, dtype=jnp.int32)
    upto = jnp.sum(enc_rows[:, None, :] <= docs[:, :, -1:], axis=2, dtype=jnp.int32)
    low = before // 128 * 128
    steps = (upto - low + span - 1) // span
    return jnp.minimum(low, length - steps * span), steps


def attend(x, width, low, steps, dec_rows, enc_rows):
    group, _, count = x.shape
    rows = low.shape[0]
    length = group * count
    heads = width // HEAD_DIM
    return pl.pallas_call(
        functools.partial(attend_kernel, heads),
        grid_spec=pltpu.PrefetchScalarGridSpec(
            num_scalar_prefetch=2,
            grid=(rows,),
            in_specs=[
                pl.BlockSpec((group, 3 * width, count), lambda r, *_: (0, r, 0)),
                pl.BlockSpec((1, 1, length), lambda r, *_: (r, 0, 0)),
                pl.BlockSpec((1, 1, length), lambda r, *_: (r, 0, 0)),
            ],
            out_specs=pl.BlockSpec((group, 1, width, count), lambda r, *_: (0, r, 0, 0)),
            scratch_shapes=[
                pltpu.VMEM((HEAD_DIM + DOCS, length), jnp.bfloat16),
                pltpu.VMEM((length, HEAD_DIM + DOCS), jnp.bfloat16),
                pltpu.VMEM((HEAD_DIM, length), jnp.bfloat16),
            ],
        ),
        out_shape=jax.ShapeDtypeStruct((group, rows, width, count), x.dtype),
        cost_estimate=pl.CostEstimate(
            flops=rows * heads * length * length * 128,
            bytes_accessed=8 * rows * width * length,
            transcendentals=rows * heads * length * length // 4,
        ),
    )(low, steps, x, dec_rows[:, None, :], enc_rows[:, None, :])


def local(queries, enc_keys, enc_values, dec_ids, enc_ids):
    group = lax.axis_size("seq")
    rows, count, features = queries.shape
    width = features // group
    early = max(1, rows * 5 // 8)
    cuts = [(0, early), (early, rows - early)] if rows > 1 else [(0, rows)]
    ids = jnp.concatenate([dec_ids, enc_ids], axis=0).astype(queries.dtype)

    def exchange(block):
        return lax.all_to_all(block, "seq", split_axis=0, concat_axis=0, tiled=True)

    packed = pack(queries, enc_keys, enc_values, ids, group, *cuts[0], True)
    if group > 1 and rows > 1:
        whole, packed = deliver(packed, queries, enc_keys, enc_values, *cuts[1])
        arrived = [whole, exchange(packed)]
    else:
        arrived = [exchange(packed)]
        arrived += [exchange(pack(queries, enc_keys, enc_values, ids, group, *cut, False)) for cut in cuts[1:]]
    spread = arrived[0][:, early * 3 * width :].astype(jnp.int32)
    whole_rows = spread.transpose(1, 0, 2).reshape(2 * rows, group * count)
    dec_rows, enc_rows = whole_rows[:rows], whole_rows[rows:]
    known = (*tables(dec_rows, enc_rows), dec_rows, enc_rows)
    out = None
    for (first, size), block in zip(cuts, arrived):
        attended = attend(block, width, *[table[first : first + size] for table in known])
        out = unpack(exchange(attended), out, first, rows)
    return out


def solution(mesh):
    in_specs = (
        P("dp", "seq", None),
        P("dp", "seq", None),
        P("dp", "seq", None),
        P("dp", "seq"),
        P("dp", "seq"),
    )
    out_specs = P("dp", "seq", None)
    return jax.shard_map(local, mesh=mesh, in_specs=in_specs, out_specs=out_specs, check_vma=False)
```

```python
import functools

import jax
import jax.numpy as jnp
from jax import lax
from jax.experimental import pallas as pl
from jax.experimental.pallas import tpu as pltpu
from jax.sharding import PartitionSpec as P

HEAD_DIM = 64
DOCS = 16
SPAN = 256
MASKED = -8192.0


def pack_kernel(rows, q_ref, k_ref, v_ref, ids_ref, o_ref):
    group, _, count = o_ref.shape
    width = q_ref.shape[2] // group

    @pl.when(pl.program_id(0) < rows)
    def _():
        for slot, ref in enumerate((q_ref, k_ref, v_ref)):
            o_ref[:, slot * width : (slot + 1) * width] = ref[0].T.reshape(group, width, count)

    @pl.when(pl.program_id(0) == rows)
    def _():
        for target in range(group):
            o_ref[target, : ids_ref.shape[0]] = ids_ref[...]


def pack(q, k, v, ids, group, first, rows, with_ids):
    _, count, features = q.shape
    width = features // group
    spec = pl.BlockSpec((1, count, features), lambda r: (jnp.minimum(r, rows - 1) + first, 0, 0))
    more = ids.shape[0] if with_ids else 0
    return pl.pallas_call(
        functools.partial(pack_kernel, rows),
        grid=(rows + 1 if with_ids else rows,),
        in_specs=[spec] * 3 + [pl.BlockSpec(ids.shape, lambda r: (0, 0))],
        out_specs=pl.BlockSpec((group, 3 * width, count), lambda r: (0, r, 0)),
        out_shape=jax.ShapeDtypeStruct((group, rows * 3 * width + more, count), q.dtype),
        cost_estimate=pl.CostEstimate(
            flops=4 * rows * count * features, bytes_accessed=12 * rows * count * features, transcendentals=0
        ),
    )(q, k, v, ids)


def deliver_kernel(group, x_ref, q_ref, k_ref, v_ref, o_ref, p_ref, held, own_sem, send_sem, recv_sem):
    me = lax.axis_index("seq")

    def transfer(shift):
        target = lax.rem(me + shift, group)
        return pltpu.make_async_remote_copy(
            src_ref=x_ref.at[target],
            dst_ref=o_ref.at[me],
            send_sem=send_sem.at[shift - 1],
            recv_sem=recv_sem.at[shift - 1],
            device_id={"seq": target},
            device_id_type=pl.DeviceIdType.MESH,
        )

    @pl.when(pl.program_id(0) == 0)
    def _():
        barrier = pltpu.get_barrier_semaphore()
        for shift in range(1, group):
            pl.semaphore_signal(
                barrier, inc=1, device_id={"seq": lax.rem(me + shift, group)}, device_id_type=pl.DeviceIdType.MESH
            )
        pl.semaphore_wait(barrier, group - 1)
        for shift in sorted(range(1, group), key=lambda shift: abs(2 * shift - group)):
            transfer(shift).start()
        own = pltpu.make_async_copy(x_ref.at[me], held, own_sem)
        own.start()
        own.wait()
        own = pltpu.make_async_copy(held, o_ref.at[me], own_sem)
        own.start()
        own.wait()

    _, _, count = p_ref.shape
    width = q_ref.shape[2] // group
    for slot, ref in enumerate((q_ref, k_ref, v_ref)):
        p_ref[:, slot * width : (slot + 1) * width] = ref[0].T.reshape(group, width, count)

    @pl.when(pl.program_id(0) == pl.num_programs(0) - 1)
    def _():
        for shift in range(1, group):
            transfer(shift).wait()


def deliver(x, q, k, v, first, rows):
    group = x.shape[0]
    _, count, features = q.shape
    width = features // group
    spec = pl.BlockSpec((1, count, features), lambda r: (r + first, 0, 0))
    return pl.pallas_call(
        functools.partial(deliver_kernel, group),
        grid=(rows,),
        in_specs=[pl.BlockSpec(memory_space=pl.ANY)] + [spec] * 3,
        out_specs=(
            pl.BlockSpec(memory_space=pl.ANY),
            pl.BlockSpec((group, 3 * width, count), lambda r: (0, r, 0)),
        ),
        out_shape=(
            jax.ShapeDtypeStruct(x.shape, x.dtype),
            jax.ShapeDtypeStruct((group, rows * 3 * width, count), x.dtype),
        ),
        scratch_shapes=[
            pltpu.VMEM(x.shape[1:], x.dtype),
            pltpu.SemaphoreType.DMA,
            pltpu.SemaphoreType.DMA((group - 1,)),
            pltpu.SemaphoreType.DMA((group - 1,)),
        ],
        compiler_params=pltpu.CompilerParams(collective_id=0, has_side_effects=True),
    )(x, q, k, v)


def unpack_kernel(x_ref, *rest):
    o_ref = rest[-1]
    group, _, width, count = x_ref.shape
    o_ref[0] = x_ref[:, 0].reshape(group * width, count).T


def unpack(x, held, first, total):
    group, rows, width, count = x.shape
    args = (x,) if held is None else (x, held)
    in_specs = [pl.BlockSpec((group, 1, width, count), lambda r: (0, r, 0, 0))]
    if held is not None:
        in_specs.append(pl.BlockSpec(memory_space=pl.ANY))
    return pl.pallas_call(
        unpack_kernel,
        grid=(rows,),
        in_specs=in_specs,
        out_specs=pl.BlockSpec((1, count, group * width), lambda r: (r + first, 0, 0)),
        out_shape=jax.ShapeDtypeStruct((total, count, group * width), x.dtype),
        input_output_aliases={} if held is None else {1: 0},
        cost_estimate=pl.CostEstimate(
            flops=4 * rows * count * group * width, bytes_accessed=4 * rows * count * group * width, transcendentals=0
        ),
    )(*args)


def attend_kernel(heads, low_ref, high_ref, x_ref, dec_ref, enc_ref, o_ref, q_all, k_all, v_all):
    group, stacked, count = x_ref.shape
    width = stacked // 3
    length = group * count
    row = pl.program_id(0)
    span = min(SPAN, length)
    documents = lax.broadcasted_iota(jnp.int32, (DOCS, length), 0)
    dec_hot = jnp.where(documents == dec_ref[0], 1.0, 0.0).astype(jnp.bfloat16)
    enc_miss = jnp.where(documents == enc_ref[0], 0.0, MASKED).astype(jnp.bfloat16)
    for head in range(heads):
        place = pl.ds(head * HEAD_DIM, HEAD_DIM)
        for part in range(group):
            columns = pl.ds(part * count, count)
            q_all[:HEAD_DIM, columns] = x_ref[part, place]
            v_all[:, columns] = x_ref[part, pl.ds(2 * width + head * HEAD_DIM, HEAD_DIM)]
        q_all[HEAD_DIM:, :] = dec_hot
        for part in range(group):
            columns = slice(part * count, (part + 1) * count)
            both = jnp.concatenate([x_ref[part, pl.ds(width + head * HEAD_DIM, HEAD_DIM)], enc_miss[:, columns]], axis=0)
            k_all[columns, :] = both.T

        def one_span(block):
            at = pl.multiple_of(block * span, span)
            query = q_all[:, pl.ds(at, span)]
            low = low_ref[row, block]
            steps = high_ref[row, block]

            def step(index, held):
                peak, total, summed = held
                start = pl.multiple_of(low + index * span, 128)
                scores = jnp.dot(
                    k_all[pl.ds(start, span), :], query, preferred_element_type=jnp.float32
                )
                fresh = jnp.maximum(peak, jnp.max(scores, axis=0, keepdims=True))
                scale = jnp.exp(peak - fresh)
                expos = jnp.exp(scores - fresh)
                total = total * scale + jnp.sum(expos, axis=0, keepdims=True)
                summed = summed * scale + jnp.dot(
                    v_all[:, pl.ds(start, span)], expos.astype(jnp.bfloat16), preferred_element_type=jnp.float32
                )
                return fresh, total, summed

            init = (
                jnp.full((1, span), 4 * MASKED, jnp.float32),
                jnp.zeros((1, span), jnp.float32),
                jnp.zeros((HEAD_DIM, span), jnp.float32),
            )
            _, total, summed = lax.fori_loop(0, steps, step, init)
            return (summed / total).astype(jnp.bfloat16)

        if count == span:

            def each(block, carry):
                o_ref[block, 0, place] = one_span(block)
                return carry

            lax.fori_loop(0, length // span, each, 0)
        else:
            for block in range(length // span):
                result = one_span(block)
                for piece in range(0, span, count):
                    at = block * span + piece
                    width_here = min(count, span)
                    o_ref[at // count, 0, place, pl.ds(at % count, width_here)] = result[:, piece : piece + width_here]


def tables(dec_rows, enc_rows):
    rows, length = dec_rows.shape
    span = min(SPAN, length)
    docs = dec_rows.reshape(rows, length // span, span)
    before = jnp.sum(enc_rows[:, None, :] < docs[:, :, :1], axis=2, dtype=jnp.int32)
    upto = jnp.sum(enc_rows[:, None, :] <= docs[:, :, -1:], axis=2, dtype=jnp.int32)
    low = before // 128 * 128
    steps = (upto - low + span - 1) // span
    return jnp.minimum(low, length - steps * span), steps


def attend(x, width, low, steps, dec_rows, enc_rows):
    group, _, count = x.shape
    rows = low.shape[0]
    length = group * count
    heads = width // HEAD_DIM
    return pl.pallas_call(
        functools.partial(attend_kernel, heads),
        grid_spec=pltpu.PrefetchScalarGridSpec(
            num_scalar_prefetch=2,
            grid=(rows,),
            in_specs=[
                pl.BlockSpec((group, 3 * width, count), lambda r, *_: (0, r, 0)),
                pl.BlockSpec((1, 1, length), lambda r, *_: (r, 0, 0)),
                pl.BlockSpec((1, 1, length), lambda r, *_: (r, 0, 0)),
            ],
            out_specs=pl.BlockSpec((group, 1, width, count), lambda r, *_: (0, r, 0, 0)),
            scratch_shapes=[
                pltpu.VMEM((HEAD_DIM + DOCS, length), jnp.bfloat16),
                pltpu.VMEM((length, HEAD_DIM + DOCS), jnp.bfloat16),
                pltpu.VMEM((HEAD_DIM, length), jnp.bfloat16),
            ],
        ),
        out_shape=jax.ShapeDtypeStruct((group, rows, width, count), x.dtype),
        cost_estimate=pl.CostEstimate(
            flops=rows * heads * length * length * 128,
            bytes_accessed=8 * rows * width * length,
            transcendentals=rows * heads * length * length // 4,
        ),
    )(low, steps, x, dec_rows[:, None, :], enc_rows[:, None, :])


def local(queries, enc_keys, enc_values, dec_ids, enc_ids):
    group = lax.axis_size("seq")
    rows, count, features = queries.shape
    width = features // group
    early = max(1, rows * 5 // 8)
    cuts = [(0, early), (early, rows - early)] if rows > 1 else [(0, rows)]
    ids = jnp.concatenate([dec_ids, enc_ids], axis=0).astype(queries.dtype)

    def exchange(block):
        return lax.all_to_all(block, "seq", split_axis=0, concat_axis=0, tiled=True)

    packed = pack(queries, enc_keys, enc_values, ids, group, *cuts[0], True)
    if group > 1 and rows > 1:
        whole, packed = deliver(packed, queries, enc_keys, enc_values, *cuts[1])
        arrived = [whole, exchange(packed)]
    else:
        arrived = [exchange(packed)]
        arrived += [exchange(pack(queries, enc_keys, enc_values, ids, group, *cut, False)) for cut in cuts[1:]]
    spread = arrived[0][:, early * 3 * width :].astype(jnp.int32)
    whole_rows = spread.transpose(1, 0, 2).reshape(2 * rows, group * count)
    dec_rows, enc_rows = whole_rows[:rows], whole_rows[rows:]
    known = (*tables(dec_rows, enc_rows), dec_rows, enc_rows)
    out = None
    for (first, size), block in zip(cuts, arrived):
        attended = attend(block, width, *[table[first : first + size] for table in known])
        out = unpack(exchange(attended), out, first, rows)
    return out


def solution(mesh):
    in_specs = (
        P("dp", "seq", None),
        P("dp", "seq", None),
        P("dp", "seq", None),
        P("dp", "seq"),
        P("dp", "seq"),
    )
    out_specs = P("dp", "seq", None)
    return jax.shard_map(local, mesh=mesh, in_specs=in_specs, out_specs=out_specs, check_vma=False)
```
